32 devices in a mesh: fsdp: 8 (over z, y), tp: 4 (over x, core).
Axes of the slice: x: 2, y: 2, z: 4, core: 2. Of those that a mesh axis runs over, the one named last changes fastest.
Arguments:
- block_in: bfloat16 [8192, 2048], P(('fsdp', 'tp')), may hold values from -6 to 6
- segment_ids: int32 [8192], P('fsdp'), may hold values from 0 to 31, never falling along the last dimension, each value on 1 to 512 neighbouring positions
- w_query: bfloat16 [2048, 2048], P('fsdp', 'tp'), may hold values from -0.125 to 0.125
- w_key: bfloat16 [2048, 2048], P('fsdp', 'tp'), may hold values from -0.125 to 0.125
- w_value: bfloat16 [2048, 2048], P('fsdp', 'tp'), may hold values from -0.125 to 0.125
- w_out: bfloat16 [2048, 2048], P('fsdp', 'tp'), may hold values from -0.125 to 0.125
- w_gate: bfloat16 [2048, 8192], P('fsdp', 'tp'), may hold values from -0.125 to 0.125
- w_up: bfloat16 [2048, 8192], P('fsdp', 'tp'), may hold values from -0.125 to 0.125
- w_down: bfloat16 [2048, 8192], P('fsdp', 'tp'), may hold values from -0.0625 to 0.0625
- gains: bfloat16 [4, 2048], replicated, may hold values from 0.25 to 1.75
- out_cotangent: bfloat16 [8192, 2048], P(('fsdp', 'tp')), may hold values from -18 to 18
Outputs:
- block_out: bfloat16 [8192, 2048], P(('fsdp', 'tp'))
- input_grad: bfloat16 [8192, 2048], P(('fsdp', 'tp'))
- query_grad: float32 [2048, 2048], P('fsdp', 'tp')
- key_grad: float32 [2048, 2048], P('fsdp', 'tp')
- value_grad: float32 [2048, 2048], P('fsdp', 'tp')
- output_grad: float32 [2048, 2048], P('fsdp', 'tp')
- gate_grad: float32 [2048, 8192], P('fsdp', 'tp')
- up_grad: float32 [2048, 8192], P('fsdp', 'tp')
- down_grad: float32 [2048, 8192], P('fsdp', 'tp')
- gains_grad: float32 [4, 2048], replicated
The draws below stay inside these ranges and needn't reach their ends.
Inputs may be any that keep to these rules, and one draw needn't show every extreme that they name: `segment_ids`: segment ids never fall along the tokens; a segment covers 1 to 512 consecutive tokens.
All inputs are finite; a program needn't handle non-finite values.
Results may differ from the reference program's by a relative error of at most 0.02.
Values may be sent and summed in bfloat16 or wider, within the bound.
A program may use at most 192 MiB of HBM per device.

```python
import math
import jax
import jax.numpy as jnp
import numpy as np
from jax import lax

D = 2048
H = 16
HD = 128
FF = 8192
LEN = 1024
TOKENS = 8192


def draw_out_cotangent(key, part):
    row_share = jnp.arange(TOKENS, dtype=jnp.float32)[:, None] / TOKENS
    basic_draw = jax.random.truncated_normal(key, -6.0, 6.0, (TOKENS, D), jnp.float32)
    factor = 1.0 + 2.0 * row_share
    return (basic_draw * factor).astype(jnp.bfloat16)


def level_of(stream_key, shape, pieces, low, top_value):
    factor_of, own = 1.0, jax.random.fold_in(stream_key, 6)
    for position, parts in pieces:
        heights = jnp.exp(jax.random.uniform(jax.random.fold_in(own, position), (parts,), jnp.float32, low / len(pieces), top_value / len(pieces)))
        factor_of = factor_of * jnp.repeat(heights, shape[position] // parts).reshape([-1 if axis == position else 1 for axis in range(len(shape))])
    return factor_of


def split_up(amount, total, limit, skew):
    weights = [(1 << 20) // math.isqrt(rank ** skew) + 1 for rank in range(2, amount + 1)]
    surplus, given = total - limit - (amount - 1), [1] * (amount - 1)
    while surplus > 0:
        candidates = [i for i in range(amount - 1) if given[i] < limit]
        pool, remaining = sum([weights[i] for i in candidates]), surplus
        for i in candidates:
            extra = min(limit - given[i], max(1, remaining * weights[i] // pool), surplus)
            given[i] = given[i] + extra
            surplus = surplus - extra
    return np.array([limit] + given)


def ragged(rng, amount, total, limit, lean):
    if amount == 2:
        one = jax.random.randint(rng, (), max(1, total - limit), min(limit, total - 1) + 1)
        return jnp.stack([one, total - one])
    lengths = jnp.asarray(split_up(amount, total, limit, lean), jnp.int32)
    twos = (amount - 1) // 2
    donor, receiver = lengths[1:1 + 2 * twos:2], lengths[2:2 + 2 * twos:2]
    room = jnp.minimum(donor - 1, limit - receiver)
    passed = jax.random.randint(jax.random.fold_in(rng, 1), (twos,), 0, 1 << 20) % (room + 1)
    lengths = lengths.at[1:1 + 2 * twos:2].set(donor - passed).at[2:2 + 2 * twos:2].set(receiver + passed)
    return lengths[jax.random.permutation(jax.random.fold_in(rng, 2), amount)]


def noise(rng, extent, width, bound, cuts=(), kind=jnp.bfloat16):
    result = jax.random.normal(rng, extent, jnp.float32) * width
    if len(cuts) > 0:
        result = level_of(rng, extent, cuts, -0.22, 0.18) * result
    return jnp.clip(result, min=-bound, max=bound).astype(kind)


def setup_inputs(seed: int = 0) -> dict:
    streams_of = jax.random.split(jax.random.key(seed), 12)
    return {
        "block_in": noise(streams_of[0], (TOKENS, D), 1.0, 6.0, ((0, 32),)),
        "segment_ids": jnp.searchsorted(jnp.cumsum(ragged(streams_of[1], TOKENS * 4 // LEN, TOKENS, LEN // 2, 1)), jnp.arange(TOKENS), side="right").astype(jnp.int32),
        "w_query": noise(streams_of[2], (D, D), D ** -0.5, 0.125, ((0, 8), (1, 4))),
        "w_key": noise(streams_of[3], (D, D), D ** -0.5, 0.125, ((0, 8), (1, 4))),
        "w_value": noise(streams_of[4], (D, D), D ** -0.5, 0.125, ((0, 8), (1, 4))),
        "w_out": noise(streams_of[5], (D, D), D ** -0.5, 0.125, ((0, 8), (1, 4))),
        "w_gate": noise(streams_of[6], (D, FF), D ** -0.5, 0.125, ((0, 8), (1, 4))),
        "w_up": noise(streams_of[7], (D, FF), D ** -0.5, 0.125, ((0, 8), (1, 4))),
        "w_down": noise(streams_of[8], (D, FF), FF ** -0.5, 0.0625, ((0, 8), (1, 4))),
        "gains": jnp.clip(1.0 + 0.15 * jax.random.normal(streams_of[9], (4, D), jnp.float32), 0.25, 1.75).astype(jnp.bfloat16),
        "out_cotangent": draw_out_cotangent(jax.random.fold_in(streams_of[11], 71), 0),
    }


EPSILON = 1e-06
THETA = 500000.0
NEG_LARGE = -1e+30
HIGHEST = lax.Precision.HIGHEST

@jax.custom_vjp
def low(v):
    return lax.optimization_barrier(v.astype(jnp.bfloat16)).astype(jnp.float32)

@jax.custom_vjp
def low_back(v):
    return v

def low_keep(v):
    return (low(v), None)

def low_pass(kept, grad):
    return (grad,)

def back_keep(v):
    return (v, None)

def back_low(kept, grad):
    return (low(grad),)
low.defvjp(low_keep, low_pass)
low_back.defvjp(back_keep, back_low)

def matmul(left, right):
    return jnp.dot(left, right, precision=HIGHEST, preferred_element_type=jnp.float32)

def row_scale(values):
    return lax.rsqrt(lax.optimization_barrier(jnp.mean(values * values, axis=-1, keepdims=True)) + EPSILON)

def rotate_half(values):
    front_half = values[..., :HD // 2]
    back_half = values[..., HD // 2:]
    return jnp.concatenate([-back_half, front_half], axis=-1)

def rotary(values, cosine, sine):
    return values * cosine + rotate_half(values) * sine

def sequence_forward(params, seq_in, seq_ids):
    w_query, w_key, w_value, w_out, w_gate, w_up, w_down, gain_rows = params
    positions = jnp.arange(LEN, dtype=jnp.int32)
    freq_index = jnp.arange(HD // 2, dtype=jnp.float32)
    frequency = THETA ** (-2.0 * freq_index / HD)
    angles = positions.astype(jnp.float32)[:, None] * frequency[None, :]
    angles = jnp.concatenate([angles, angles], axis=1)[:, None, :]
    cosine = jnp.cos(angles)
    sine = jnp.sin(angles)
    query_raw = low_back(matmul(seq_in, w_query))
    key_raw = low_back(matmul(seq_in, w_key))
    value_low = low_back(low(matmul(seq_in, w_value))).reshape(LEN, H, HD)
    query_unit = query_raw * row_scale(query_raw) * gain_rows[0]
    key_unit = key_raw * row_scale(key_raw) * gain_rows[1]
    query_rot = low(rotary(query_unit.reshape(LEN, H, HD), cosine, sine))
    key_rot = low(rotary(key_unit.reshape(LEN, H, HD), cosine, sine))
    scores = jnp.einsum('qhd,khd->hqk', query_rot, key_rot, precision=HIGHEST, preferred_element_type=jnp.float32)
    scores = low_back(scores * HD ** (-0.5))
    visible = (seq_ids[:, None] == seq_ids[None, :]) & (positions[None, :] <= positions[:, None])
    scores = jnp.where(visible[None, :, :], scores, NEG_LARGE)
    probs_low = low(jax.nn.softmax(scores, axis=-1))
    context = jnp.einsum('hqk,khd->qhd', probs_low, value_low, precision=HIGHEST, preferred_element_type=jnp.float32)
    context = low_back(low(context)).reshape(LEN, D)
    attention = low_back(matmul(context, w_out.T))
    hidden = seq_in + attention * row_scale(attention) * gain_rows[2]
    hidden_low = low(hidden)
    gate = low_back(matmul(hidden_low, w_gate))
    up_value = low_back(matmul(hidden_low, w_up))
    inner = low(jax.nn.silu(gate) * up_value)
    mixed = low_back(matmul(inner, w_down.T))
    return hidden + mixed * row_scale(mixed) * gain_rows[3]

def reference(block_in, segment_ids, w_query, w_key, w_value, w_out, w_gate, w_up, w_down, gains, out_cotangent):
    params = tuple((weight_array.astype(jnp.float32) for weight_array in (w_query, w_key, w_value, w_out, w_gate, w_up, w_down, gains)))
    seq_count = TOKENS // LEN
    inputs = block_in.astype(jnp.float32).reshape(seq_count, LEN, D)
    all_ids = segment_ids.reshape(seq_count, LEN)
    checkpointed = jax.checkpoint(sequence_forward)

    def forward(param_tuple, input_seqs):

        def one_sequence(pair):
            return checkpointed(param_tuple, pair[0], pair[1])
        return lax.map(one_sequence, (input_seqs, all_ids))
    outputs, pullback = jax.vjp(forward, params, inputs)
    cotangent = out_cotangent.astype(jnp.float32).reshape(seq_count, LEN, D)
    param_grads, input_grad = pullback(cotangent)
    return (outputs.reshape(TOKENS, D).astype(jnp.bfloat16), input_grad.reshape(TOKENS, D).astype(jnp.bfloat16), param_grads[0], param_grads[1], param_grads[2], param_grads[3], param_grads[4], param_grads[5], param_grads[6], param_grads[7])
```

```python
import functools

import jax
import jax.numpy as jnp
import numpy as np
from jax import lax
from jax.experimental import pallas as pl
from jax.experimental.pallas import tpu as pltpu
from jax.sharding import PartitionSpec as P

HD = 128
LEN = 1024
SEG_MAX = 512
BLOCK = 256

EPSILON = 1e-06
THETA = 500000.0
NEG_LARGE = -1e30
F32 = jnp.float32
BF16 = jnp.bfloat16


def dot_plain(left, right):
    return jnp.dot(left, right, preferred_element_type=F32)


def dot_rows(left, right):
    return lax.dot_general(left, right, (((1,), (1,)), ((), ())), preferred_element_type=F32)


def dot_cols(left, right):
    return lax.dot_general(left, right, (((0,), (0,)), ((), ())), preferred_element_type=F32)


def ring_order(n):
    return [i for i in range(0, n, 2)] + [i for i in range(n - 1, 0, -2)]


class Ring:
    def __init__(self, n):
        order = ring_order(n)
        place = {f: p for p, f in enumerate(order)}
        self.n, self.half = n, n // 2
        self.right = [(order[p], order[(p + 1) % n]) for p in range(n)]
        self.left = [(order[(p + 1) % n], order[p]) for p in range(n)]
        table = np.array([[order[(place[f] + k) % n] for k in range(n)] for f in range(n)], np.int32)
        self.owners = lax.dynamic_slice_in_dim(jnp.asarray(table), lax.axis_index("fsdp"), 1, 0)[0]

    def owner(self, k):
        return self.owners[k % self.n]

    def send_right(self, x):
        return lax.ppermute(x, "fsdp", self.right)

    def send_left(self, x):
        return lax.ppermute(x, "fsdp", self.left)


def ring_gather(ring, shard, name):
    rows, cols = shard.shape
    mid = rows // 2
    full = jnp.zeros((ring.n * rows, cols), shard.dtype)

    def put(full, block, k, skip=0):
        return lax.dynamic_update_slice(full, block, (ring.owner(k) * rows + skip, jnp.int32(0)))

    full = put(full, shard, 0)
    ahead = behind = shard
    for k in range(1, ring.half):
        with jax.named_scope(f"{name}_r{k}"):
            behind = ring.send_right(behind)
        with jax.named_scope(f"{name}_l{k}"):
            ahead = ring.send_left(ahead)
        full = put(full, behind, -k)
        full = put(full, ahead, k)
    with jax.named_scope(f"{name}_r{ring.half}"):
        behind = ring.send_right(behind[:mid])
    with jax.named_scope(f"{name}_l{ring.half}"):
        ahead = ring.send_left(ahead[mid:])
    full = put(full, behind, ring.half)
    full = put(full, ahead, ring.half, mid)
    return full


def ring_scatter(ring, terms, name):
    rows = terms.shape[0] // ring.n
    mid = rows // 2

    def part(k, skip=0, count=rows):
        start = ring.owner(k) * rows + skip
        return lax.dynamic_slice_in_dim(terms, start, count, 0).astype(F32)

    with jax.named_scope(f"{name}_r{ring.half}"):
        from_left = ring.send_right(part(ring.half, 0, mid).astype(BF16))
    with jax.named_scope(f"{name}_l{ring.half}"):
        from_right = ring.send_left(part(-ring.half, mid, mid).astype(BF16))
    for k in range(ring.half - 1, 0, -1):
        if k == ring.half - 1:
            from_left = jnp.pad(from_left, ((0, mid), (0, 0)))
            from_right = jnp.pad(from_right, ((mid, 0), (0, 0)))
        go_right = (part(k) + from_left.astype(F32)).astype(BF16)
        go_left = (part(-k) + from_right.astype(F32)).astype(BF16)
        with jax.named_scope(f"{name}_r{k}"):
            from_left = ring.send_right(go_right)
        with jax.named_scope(f"{name}_l{k}"):
            from_right = ring.send_left(go_left)
    return part(0) + from_left.astype(F32) + from_right.astype(F32)


def tp_pairs(size, bit):
    return [(i, i ^ bit) for i in range(size)]


def tp_swap(x, size, bit):
    return lax.ppermute(x, "tp", tp_pairs(size, bit))


def gather_rows(own, size):
    far = tp_swap(own, size, 2)
    near = tp_swap(own, size, 1)
    corner = tp_swap(far, size, 1)
    return jnp.concatenate([own, near, far, corner], axis=0)


def scatter_rows(terms, size):
    rows = terms.shape[0] // size
    blocks = [terms[j * rows : (j + 1) * rows] for j in range(size)]
    far_in = tp_swap(blocks[3], size, 1)
    go_far = (blocks[2].astype(F32) + far_in.astype(F32)).astype(BF16)
    far = tp_swap(go_far, size, 2)
    near = tp_swap(blocks[1], size, 1)
    return blocks[0].astype(F32) + near.astype(F32) + far.astype(F32)


def sum_rows(values, size):
    m, total = values.shape
    v = values.reshape(m, size, total // size)
    bit = 1
    while bit < size:
        got = tp_swap(v, size, bit)
        v = v + got[:, np.arange(size) ^ bit]
        bit *= 2
    return v.reshape(m, total)


def sum_all(values, n, size):
    bit = 1
    while bit < size:
        values = values + tp_swap(values, size, bit)
        bit *= 2
    bit = 1
    while bit < n:
        values = values + lax.ppermute(values, "fsdp", [(i, i ^ bit) for i in range(n)])
        bit *= 2
    return values


def rel_block(t, c, rows):
    return pl.ds(pl.multiple_of((t ^ c) * rows, rows), rows)


def in_order(ref, t, count, rows):
    return jnp.concatenate([ref[rel_block(t, c, rows), :] for c in range(count)], axis=0)


def visible_block(c, lo, hi, ids_col, ids_row):
    q_pos = c * BLOCK + lax.broadcasted_iota(jnp.int32, (BLOCK, hi - lo), 0)
    k_pos = lo + lax.broadcasted_iota(jnp.int32, (BLOCK, hi - lo), 1)
    same = ids_col[c * BLOCK : (c + 1) * BLOCK, :] == ids_row[:, lo:hi]
    return same & (k_pos <= q_pos)


def key_range(c):
    first = max(0, c * BLOCK - SEG_MAX + 1) // BLOCK * BLOCK
    return first, (c + 1) * BLOCK


def attend_kernel(count, rows, t_ref, ids_col, ids_row, q_ref, k_ref, v_ref, ctx_ref, lse_ref):
    t = t_ref[0]
    q = in_order(q_ref, t, count, rows)
    k = in_order(k_ref, t, count, rows)
    v = in_order(v_ref, t, count, rows)
    per = rows // BLOCK
    for c in range(count * per):
        lo, hi = key_range(c)
        at = pl.ds(pl.multiple_of((t ^ (c // per)) * rows + c % per * BLOCK, BLOCK), BLOCK)
        scores = dot_rows(q[c * BLOCK : (c + 1) * BLOCK], k[lo:hi]) * HD ** (-0.5)
        scores = jnp.where(visible_block(c, lo, hi, ids_col, ids_row), scores, NEG_LARGE)
        top = jnp.max(scores, axis=-1, keepdims=True)
        exponent = jnp.exp(scores - top)
        total = jnp.sum(exponent, axis=-1, keepdims=True)
        probs = (exponent * (1.0 / total)).astype(BF16)
        ctx_ref[at, :] = dot_plain(probs, v[lo:hi]).astype(BF16)
        lse_ref[0, at, :] = top + jnp.log(total)


def attend_back_kernel(
    count, rows, t_ref, ids_col, ids_row, q_ref, k_ref, v_ref, g_ref, lse_ref, dq_ref, dk_ref, dv_ref, dk_acc, dv_acc
):
    t = t_ref[0]
    q = in_order(q_ref, t, count, rows)
    k = in_order(k_ref, t, count, rows)
    v = in_order(v_ref, t, count, rows)
    g = in_order(g_ref, t, count, rows)
    dk_acc[...] = jnp.zeros_like(dk_acc)
    dv_acc[...] = jnp.zeros_like(dv_acc)
    per = rows // BLOCK
    for c in range(count * per):
        lo, hi = key_range(c)
        at = pl.ds(pl.multiple_of((t ^ (c // per)) * rows + c % per * BLOCK, BLOCK), BLOCK)
        q_c, g_c = q[c * BLOCK : (c + 1) * BLOCK], g[c * BLOCK : (c + 1) * BLOCK]
        scores = dot_rows(q_c, k[lo:hi]) * HD ** (-0.5)
        seen = visible_block(c, lo, hi, ids_col, ids_row)
        probs = jnp.where(seen, jnp.exp(jnp.where(seen, scores, NEG_LARGE) - lse_ref[0, at, :]), 0.0)
        probs_back = dot_rows(g_c, v[lo:hi])
        delta = jnp.sum(probs * probs_back, axis=-1, keepdims=True)
        scores_back = (probs * (probs_back - delta)).astype(BF16)
        dq_ref[at, :] = dot_plain(scores_back, k[lo:hi]) * HD ** (-0.5)
        dk_acc[lo:hi, :] += dot_cols(scores_back, q_c)
        dv_acc[lo:hi, :] += dot_cols(probs.astype(BF16), g_c)
    for c in range(count):
        dk_ref[rel_block(t, c, rows), :] = dk_acc[c * rows : (c + 1) * rows, :] * HD ** (-0.5)
        dv_ref[rel_block(t, c, rows), :] = dv_acc[c * rows : (c + 1) * rows, :].astype(BF16)


def attention_forward(t, ids, q, k, v, count):
    length, width = q.shape
    heads = width // HD
    col = pl.BlockSpec((length, HD), lambda h, t: (0, h))
    spec = pltpu.PrefetchScalarGridSpec(
        num_scalar_prefetch=1,
        grid=(heads,),
        in_specs=[
            pl.BlockSpec((length, 1), lambda h, t: (0, 0)),
            pl.BlockSpec((1, length), lambda h, t: (0, 0)),
            col,
            col,
            col,
        ],
        out_specs=[col, pl.BlockSpec((1, length, 1), lambda h, t: (h, 0, 0))],
    )
    return pl.pallas_call(
        functools.partial(attend_kernel, count, length // count),
        out_shape=[
            jax.ShapeDtypeStruct((length, width), BF16),
            jax.ShapeDtypeStruct((heads, length, 1), F32),
        ],
        grid_spec=spec,
        cost_estimate=pl.CostEstimate(
            flops=4 * length * length * width, bytes_accessed=8 * length * width, transcendentals=heads * length * length
        ),
        name="attend",
    )(t, ids.reshape(length, 1), ids.reshape(1, length), q, k, v)


def attention_backward(t, ids, q, k, v, g, lse, count):
    length, width = q.shape
    heads = width // HD
    col = pl.BlockSpec((length, HD), lambda h, t: (0, h))
    spec = pltpu.PrefetchScalarGridSpec(
        num_scalar_prefetch=1,
        grid=(heads,),
        in_specs=[
            pl.BlockSpec((length, 1), lambda h, t: (0, 0)),
            pl.BlockSpec((1, length), lambda h, t: (0, 0)),
            col,
            col,
            col,
            col,
            pl.BlockSpec((1, length, 1), lambda h, t: (h, 0, 0)),
        ],
        out_specs=[col, col, col],
        scratch_shapes=[pltpu.VMEM((length, HD), F32), pltpu.VMEM((length, HD), F32)],
    )
    return pl.pallas_call(
        functools.partial(attend_back_kernel, count, length // count),
        out_shape=[
            jax.ShapeDtypeStruct((length, width), F32),
            jax.ShapeDtypeStruct((length, width), F32),
            jax.ShapeDtypeStruct((length, width), BF16),
        ],
        grid_spec=spec,
        cost_estimate=pl.CostEstimate(
            flops=10 * length * length * width, bytes_accessed=18 * length * width, transcendentals=heads * length * length
        ),
        name="attend_back",
    )(t, ids.reshape(length, 1), ids.reshape(1, length), q, k, v, g, lse)


def rotate_half(values):
    front_half = values[..., : HD // 2]
    back_half = values[..., HD // 2 :]
    return jnp.concatenate([-back_half, front_half], axis=-1)


def rotate_back(values):
    front_half = values[..., : HD // 2]
    back_half = values[..., HD // 2 :]
    return jnp.concatenate([back_half, -front_half], axis=-1)


def rotary(values, cosine, sine):
    return values * cosine + rotate_half(values) * sine


def unrotary(values, cosine, sine):
    return values * cosine + rotate_back(values * sine)


def rope_tables(positions):
    freq_index = jnp.arange(HD // 2, dtype=F32)
    frequency = THETA ** (-2.0 * freq_index / HD)
    angles = positions.astype(F32)[:, None] * frequency[None, :]
    angles = jnp.concatenate([angles, angles], axis=1)[:, None, :]
    return jnp.cos(angles), jnp.sin(angles)


def norm_back(unit_rows, scales, grad_unit):
    return scales * (grad_unit - unit_rows * jnp.mean(grad_unit * unit_rows, axis=-1, keepdims=True))


def local(n, size, block_in, segment_ids, w_query, w_key, w_value, w_out, w_gate, w_up, w_down, gains, out_cotangent):
    t = lax.axis_index("tp")
    ring = Ring(n)
    model_width = block_in.shape[1]
    width = w_query.shape[1]
    heads = width // HD
    own_rows = block_in.shape[0]
    rows = own_rows * size
    assert rows == LEN and segment_ids.shape[0] == LEN
    gain_values = gains.astype(F32)
    head_gains = lax.dynamic_slice_in_dim(gain_values, t * width, width, 1)
    positions = jnp.concatenate([(t ^ j) * own_rows + jnp.arange(own_rows, dtype=jnp.int32) for j in range(size)])
    cosine, sine = rope_tables(positions)
    t_arr = t.reshape(1).astype(jnp.int32)

    attn_full = ring_gather(ring, jnp.concatenate([w_query, w_key, w_value, w_out], axis=1), "wa")
    gate_full = ring_gather(ring, w_gate, "wg")
    up_full = ring_gather(ring, w_up, "wu")
    down_full = ring_gather(ring, w_down, "wd")
    out_full = attn_full[:, 3 * width :]

    gathered_in = gather_rows(block_in, size)
    query_raw = dot_plain(gathered_in, attn_full[:, :width])
    key_raw = dot_plain(gathered_in, attn_full[:, width : 2 * width])
    value_low = dot_plain(gathered_in, attn_full[:, 2 * width : 3 * width]).astype(BF16)
    squares = sum_rows(jnp.stack([jnp.sum(query_raw * query_raw, axis=1), jnp.sum(key_raw * key_raw, axis=1)]), size)
    scales = lax.rsqrt(squares / model_width + EPSILON)
    query_scale, key_scale = scales[0][:, None], scales[1][:, None]
    query_unit = query_raw * query_scale
    key_unit = key_raw * key_scale
    query_rot = rotary((query_unit * head_gains[0]).reshape(rows, heads, HD), cosine, sine)
    key_rot = rotary((key_unit * head_gains[1]).reshape(rows, heads, HD), cosine, sine)
    query_rot = query_rot.reshape(rows, width).astype(BF16)
    key_rot = key_rot.reshape(rows, width).astype(BF16)
    context_low, lse = attention_forward(t_arr, segment_ids, query_rot, key_rot, value_low, size)
    attn_sum = scatter_rows(dot_rows(context_low, out_full).astype(BF16), size)
    attn_scale = lax.rsqrt(jnp.mean(attn_sum * attn_sum, axis=1, keepdims=True) + EPSILON)
    attn_unit = attn_sum * attn_scale
    hidden_mid = block_in.astype(F32) + attn_unit * gain_values[2]
    hidden_group = gather_rows(hidden_mid.astype(BF16), size)
    gate_raw = dot_plain(hidden_group, gate_full)
    up_raw = dot_plain(hidden_group, up_full)
    sigmoid_gate = jax.nn.sigmoid(gate_raw)
    silu_gate = gate_raw * sigmoid_gate
    inner_low = (silu_gate * up_raw).astype(BF16)
    mlp_sum = scatter_rows(dot_rows(inner_low, down_full).astype(BF16), size)
    mlp_scale = lax.rsqrt(jnp.mean(mlp_sum * mlp_sum, axis=1, keepdims=True) + EPSILON)
    mlp_unit = mlp_sum * mlp_scale
    block_out = (hidden_mid + mlp_unit * gain_values[3]).astype(BF16)

    grad_final = out_cotangent.astype(F32)
    mlp_gain_term = jnp.sum(grad_final * mlp_unit, axis=0)
    mixed_back = norm_back(mlp_unit, mlp_scale, grad_final * gain_values[3]).astype(BF16)
    mixed_group = gather_rows(mixed_back, size)
    down_grad = dot_cols(mixed_group, inner_low).astype(BF16)
    down_sum = ring_scatter(ring, down_grad, "gd")
    inner_back = dot_plain(mixed_group, down_full)
    gate_back = (inner_back * up_raw * sigmoid_gate * (1.0 + gate_raw * (1.0 - sigmoid_gate))).astype(BF16)
    up_back = (inner_back * silu_gate).astype(BF16)
    gate_grad = dot_cols(hidden_group, gate_back).astype(BF16)
    gate_sum = ring_scatter(ring, gate_grad, "gg")
    up_grad = dot_cols(hidden_group, up_back).astype(BF16)
    up_sum = ring_scatter(ring, up_grad, "gu")
    hidden_terms = dot_rows(gate_back, gate_full) + dot_rows(up_back, up_full)
    hidden_back = grad_final + scatter_rows(hidden_terms.astype(BF16), size)
    attn_gain_term = jnp.sum(hidden_back * attn_unit, axis=0)
    attention_back = norm_back(attn_unit, attn_scale, hidden_back * gain_values[2]).astype(BF16)
    attention_group = gather_rows(attention_back, size)
    context_back = dot_plain(attention_group, out_full).astype(BF16)
    output_grad = dot_cols(attention_group, context_low).astype(BF16)
    output_sum = ring_scatter(ring, output_grad, "go")
    rot_query_back, rot_key_back, value_back = attention_backward(
        t_arr, segment_ids, query_rot, key_rot, value_low, context_back, lse, size
    )
    query_norm_back = unrotary(rot_query_back.reshape(rows, heads, HD), cosine, sine).reshape(rows, width)
    key_norm_back = unrotary(rot_key_back.reshape(rows, heads, HD), cosine, sine).reshape(rows, width)
    query_gain_term = jnp.sum(query_norm_back * query_unit, axis=0)
    key_gain_term = jnp.sum(key_norm_back * key_unit, axis=0)
    query_unit_back = query_norm_back * head_gains[0]
    key_unit_back = key_norm_back * head_gains[1]
    dots = sum_rows(
        jnp.stack([jnp.sum(query_unit_back * query_unit, axis=1), jnp.sum(key_unit_back * key_unit, axis=1)]), size
    )
    query_back = (query_scale * (query_unit_back - query_unit * (dots[0] / model_width)[:, None])).astype(BF16)
    key_back = (key_scale * (key_unit_back - key_unit * (dots[1] / model_width)[:, None])).astype(BF16)
    joint_back = jnp.concatenate([query_back, key_back, value_back], axis=1)
    joint_grad = dot_cols(gathered_in, joint_back).astype(BF16)
    joint_sum = ring_scatter(ring, joint_grad, "gj")
    input_terms = dot_rows(joint_back, attn_full[:, : 3 * width])
    input_grad = (hidden_back + scatter_rows(input_terms.astype(BF16), size)).astype(BF16)

    head_terms = jnp.stack([query_gain_term, key_gain_term])
    placed = lax.dynamic_update_slice(jnp.zeros((2, model_width), F32), head_terms, (jnp.int32(0), t * width))
    gain_terms = jnp.concatenate([placed, jnp.stack([attn_gain_term, mlp_gain_term])], axis=0)
    gains_grad = sum_all(gain_terms, n, size)
    return (
        block_out,
        input_grad,
        joint_sum[:, :width],
        joint_sum[:, width : 2 * width],
        joint_sum[:, 2 * width :],
        output_sum,
        gate_sum,
        up_sum,
        down_sum,
        gains_grad,
    )


def solution(mesh):
    both = P(("fsdp", "tp"), None)
    weight = P("fsdp", "tp")
    in_specs = (both, P("fsdp"), *[weight] * 7, P(), both)
    out_specs = (both, both, *[weight] * 7, P())
    body = functools.partial(local, mesh.shape["fsdp"], mesh.shape["tp"])
    return jax.shard_map(body, mesh=mesh, in_specs=in_specs, out_specs=out_specs, check_vma=False)
```

```python
import functools

import jax
import jax.numpy as jnp
import numpy as np
from jax import lax
from jax.experimental import pallas as pl
from jax.experimental.pallas import tpu as pltpu
from jax.sharding import PartitionSpec as P

HD = 128
LEN = 1024
SEG_MAX = 512
BLOCK = 256

EPSILON = 1e-06
THETA = 500000.0
NEG_LARGE = -1e30
F32 = jnp.float32
BF16 = jnp.bfloat16


def dot_plain(left, right):
    return jnp.dot(left, right, preferred_element_type=F32)


def dot_rows(left, right):
    return lax.dot_general(left, right, (((1,), (1,)), ((), ())), preferred_element_type=F32)


def dot_cols(left, right):
    return lax.dot_general(left, right, (((0,), (0,)), ((), ())), preferred_element_type=F32)


class Place:
    def __init__(self, n, size):
        self.n, self.size, self.line, self.group = n, size, n // 2, 2 * size
        f, self.t = lax.axis_index("fsdp"), lax.axis_index("tp")
        self.a, self.y = f // 2, f % 2

    def swap(self, x, bit):
        if bit < self.size:
            return lax.ppermute(x, "tp", [(i, i ^ bit) for i in range(self.size)])
        return lax.ppermute(x, "fsdp", [(i, i ^ 1) for i in range(self.n)])

    def lines(self):
        return [[2 * a + y for a in range(self.line)] for y in (0, 1)]


def line_gather(place, mine, theirs, name):
    with jax.named_scope(f"{name}_y"):
        other = place.swap(theirs, place.size)
    first = place.y == 0
    shard = jnp.concatenate([jnp.where(first, mine, other), jnp.where(first, other, mine)], axis=0)
    with jax.named_scope(f"{name}_z"):
        return lax.all_gather(shard, "fsdp", axis=0, tiled=True, axis_index_groups=place.lines())


def line_scatter(place, terms, name):
    with jax.named_scope(f"{name}_z"):
        total = lax.psum_scatter(terms, "fsdp", scatter_dimension=0, tiled=True, axis_index_groups=place.lines())
    half = total.shape[0] // 2
    keep = lax.dynamic_slice_in_dim(total, place.y * half, half, 0)
    give = lax.dynamic_slice_in_dim(total, (1 - place.y) * half, half, 0)
    with jax.named_scope(f"{name}_y"):
        got = place.swap(give, place.size)
    first = place.y == 0
    keep, got = keep.astype(F32), got.astype(F32)
    return jnp.where(first, keep, got), jnp.where(first, got, keep)


def gather_rows(place, own, name):
    half = own.shape[0] // 2
    with jax.named_scope(f"{name}_2"):
        b2 = place.swap(own, 2)
    with jax.named_scope(f"{name}_4"):
        b4 = place.swap(own, 4)
    with jax.named_scope(f"{name}_1"):
        b1 = place.swap(own, 1)
    with jax.named_scope(f"{name}_6a"):
        b6a = place.swap(b4[:half], 2)
    with jax.named_scope(f"{name}_6b"):
        b6b = place.swap(b2[half:], 4)
    with jax.named_scope(f"{name}_3"):
        b3 = place.swap(b2, 1)
    with jax.named_scope(f"{name}_5"):
        b5 = place.swap(b4, 1)
    b6 = jnp.concatenate([b6a, b6b], axis=0)
    with jax.named_scope(f"{name}_7"):
        b7 = place.swap(b6, 1)
    return jnp.concatenate([own, b1, b2, b3, b4, b5, b6, b7], axis=0)


def scatter_rows(place, terms, name):
    rows = terms.shape[0] // place.group
    half = rows // 2
    block = [terms[j * rows : (j + 1) * rows] for j in range(place.group)]
    pair = {}
    for j in (6, 2, 4, 0):
        with jax.named_scope(f"{name}_c{j}"):
            pair[j] = block[j].astype(F32) + place.swap(block[j + 1], 1).astype(F32)
    corner = pair[6].astype(BF16)
    with jax.named_scope(f"{name}_6a"):
        via_x = place.swap(corner[:half], 2).astype(F32)
    with jax.named_scope(f"{name}_6b"):
        via_y = place.swap(corner[half:], 4).astype(F32)
    with jax.named_scope(f"{name}_2"):
        from_x = place.swap((pair[2] + jnp.pad(via_y, ((half, 0), (0, 0)))).astype(BF16), 2)
    with jax.named_scope(f"{name}_4"):
        from_y = place.swap((pair[4] + jnp.pad(via_x, ((0, half), (0, 0)))).astype(BF16), 4)
    return pair[0] + from_x.astype(F32) + from_y.astype(F32)


def sum_rows(place, values, name):
    m, total = values.shape
    v = values.reshape(m, place.group, total // place.group)
    for bit in (1, 2, 4):
        with jax.named_scope(f"{name}_{bit}"):
            got = place.swap(v, bit)
        v = v + got[:, np.arange(place.group) ^ bit]
    return v.reshape(m, total)


def sum_all(place, values):
    for bit in (1, 2, 4):
        values = values + place.swap(values, bit)
    bit = 2
    while bit < place.n:
        values = values + lax.ppermute(values, "fsdp", [(i, i ^ bit) for i in range(place.n)])
        bit *= 2
    return values


def rel_block(t, c, rows):
    return pl.ds(pl.multiple_of((t ^ c) * rows, rows), rows)


def in_order(ref, t, count, rows):
    return jnp.concatenate([ref[rel_block(t, c, rows), :] for c in range(count)], axis=0)


def visible_block(c, lo, hi, ids_col, ids_row):
    q_pos = c * BLOCK + lax.broadcasted_iota(jnp.int32, (BLOCK, hi - lo), 0)
    k_pos = lo + lax.broadcasted_iota(jnp.int32, (BLOCK, hi - lo), 1)
    same = ids_col[c * BLOCK : (c + 1) * BLOCK, :] == ids_row[:, lo:hi]
    return same & (k_pos <= q_pos)


def key_range(c):
    first = max(0, c * BLOCK - SEG_MAX + 1) // BLOCK * BLOCK
    return first, (c + 1) * BLOCK


def attend_kernel(count, rows, t_ref, ids_col, ids_row, q_ref, k_ref, v_ref, ctx_ref, lse_ref):
    t = t_ref[0]
    q = in_order(q_ref, t, count, rows)
    k = in_order(k_ref, t, count, rows)
    v = in_order(v_ref, t, count, rows)
    per = rows // BLOCK
    for c in range(count * per):
        lo, hi = key_range(c)
        at = pl.ds(pl.multiple_of((t ^ (c // per)) * rows + c % per * BLOCK, BLOCK), BLOCK)
        scores = dot_rows(q[c * BLOCK : (c + 1) * BLOCK], k[lo:hi]) * HD ** (-0.5)
        scores = jnp.where(visible_block(c, lo, hi, ids_col, ids_row), scores, NEG_LARGE)
        top = jnp.max(scores, axis=-1, keepdims=True)
        exponent = jnp.exp(scores - top)
        total = jnp.sum(exponent, axis=-1, keepdims=True)
        probs = (exponent * (1.0 / total)).astype(BF16)
        ctx_ref[at, :] = dot_plain(probs, v[lo:hi]).astype(BF16)
        lse_ref[0, at, :] = top + jnp.log(total)


def attend_back_kernel(
    count, rows, t_ref, ids_col, ids_row, q_ref, k_ref, v_ref, g_ref, lse_ref, dq_ref, dk_ref, dv_ref, dk_acc, dv_acc
):
    t = t_ref[0]
    q = in_order(q_ref, t, count, rows)
    k = in_order(k_ref, t, count, rows)
    v = in_order(v_ref, t, count, rows)
    g = in_order(g_ref, t, count, rows)
    dk_acc[...] = jnp.zeros_like(dk_acc)
    dv_acc[...] = jnp.zeros_like(dv_acc)
    per = rows // BLOCK
    for c in range(count * per):
        lo, hi = key_range(c)
        at = pl.ds(pl.multiple_of((t ^ (c // per)) * rows + c % per * BLOCK, BLOCK), BLOCK)
        q_c, g_c = q[c * BLOCK : (c + 1) * BLOCK], g[c * BLOCK : (c + 1) * BLOCK]
        scores = dot_rows(q_c, k[lo:hi]) * HD ** (-0.5)
        seen = visible_block(c, lo, hi, ids_col, ids_row)
        probs = jnp.where(seen, jnp.exp(jnp.where(seen, scores, NEG_LARGE) - lse_ref[0, at, :]), 0.0)
        probs_back = dot_rows(g_c, v[lo:hi])
        delta = jnp.sum(probs * probs_back, axis=-1, keepdims=True)
        scores_back = (probs * (probs_back - delta)).astype(BF16)
        dq_ref[at, :] = dot_plain(scores_back, k[lo:hi]) * HD ** (-0.5)
        dk_acc[lo:hi, :] += dot_cols(scores_back, q_c)
        dv_acc[lo:hi, :] += dot_cols(probs.astype(BF16), g_c)
    for c in range(count):
        dk_ref[rel_block(t, c, rows), :] = dk_acc[c * rows : (c + 1) * rows, :] * HD ** (-0.5)
        dv_ref[rel_block(t, c, rows), :] = dv_acc[c * rows : (c + 1) * rows, :].astype(BF16)


def attention_forward(t, ids, q, k, v, count):
    seqs, length = ids.shape
    width = q.shape[1]
    heads = width // HD
    col = pl.BlockSpec((length, HD), lambda s, h, t: (s, h))
    spec = pltpu.PrefetchScalarGridSpec(
        num_scalar_prefetch=1,
        grid=(seqs, heads),
        in_specs=[
            pl.BlockSpec((length, 1), lambda s, h, t: (s, 0)),
            pl.BlockSpec((pl.Squeezed(), 1, length), lambda s, h, t: (s, 0, 0)),
            col,
            col,
            col,
        ],
        out_specs=[col, pl.BlockSpec((1, length, 1), lambda s, h, t: (h, s, 0))],
    )
    return pl.pallas_call(
        functools.partial(attend_kernel, count, length // count),
        out_shape=[
            jax.ShapeDtypeStruct((seqs * length, width), BF16),
            jax.ShapeDtypeStruct((heads, seqs * length, 1), F32),
        ],
        grid_spec=spec,
        cost_estimate=pl.CostEstimate(
            flops=4 * seqs * length * length * width,
            bytes_accessed=8 * seqs * length * width,
            transcendentals=seqs * heads * length * length,
        ),
        name="attend",
    )(t, ids.reshape(-1, 1), ids.reshape(seqs, 1, length), q, k, v)


def attention_backward(t, ids, q, k, v, g, lse, count):
    seqs, length = ids.shape
    width = q.shape[1]
    heads = width // HD
    col = pl.BlockSpec((length, HD), lambda s, h, t: (s, h))
    spec = pltpu.PrefetchScalarGridSpec(
        num_scalar_prefetch=1,
        grid=(seqs, heads),
        in_specs=[
            pl.BlockSpec((length, 1), lambda s, h, t: (s, 0)),
            pl.BlockSpec((pl.Squeezed(), 1, length), lambda s, h, t: (s, 0, 0)),
            col,
            col,
            col,
            col,
            pl.BlockSpec((1, length, 1), lambda s, h, t: (h, s, 0)),
        ],
        out_specs=[col, col, col],
        scratch_shapes=[pltpu.VMEM((length, HD), F32), pltpu.VMEM((length, HD), F32)],
    )
    return pl.pallas_call(
        functools.partial(attend_back_kernel, count, length // count),
        out_shape=[
            jax.ShapeDtypeStruct((seqs * length, width), F32),
            jax.ShapeDtypeStruct((seqs * length, width), F32),
            jax.ShapeDtypeStruct((seqs * length, width), BF16),
        ],
        grid_spec=spec,
        cost_estimate=pl.CostEstimate(
            flops=10 * seqs * length * length * width,
            bytes_accessed=18 * seqs * length * width,
            transcendentals=seqs * heads * length * length,
        ),
        name="attend_back",
    )(t, ids.reshape(-1, 1), ids.reshape(seqs, 1, length), q, k, v, g, lse)


def rotate_half(values):
    front_half = values[..., : HD // 2]
    back_half = values[..., HD // 2 :]
    return jnp.concatenate([-back_half, front_half], axis=-1)


def rotate_back(values):
    front_half = values[..., : HD // 2]
    back_half = values[..., HD // 2 :]
    return jnp.concatenate([back_half, -front_half], axis=-1)


def rotary(values, cosine, sine):
    return values * cosine + rotate_half(values) * sine


def unrotary(values, cosine, sine):
    return values * cosine + rotate_back(values * sine)


def rope_tables(positions):
    freq_index = jnp.arange(HD // 2, dtype=F32)
    frequency = THETA ** (-2.0 * freq_index / HD)
    angles = positions.astype(F32)[:, None] * frequency[None, :]
    angles = jnp.concatenate([angles, angles], axis=1)[:, None, :]
    return jnp.cos(angles), jnp.sin(angles)


def norm_back(unit_rows, scales, grad_unit):
    return scales * (grad_unit - unit_rows * jnp.mean(grad_unit * unit_rows, axis=-1, keepdims=True))


def local(n, size, block_in, segment_ids, w_query, w_key, w_value, w_out, w_gate, w_up, w_down, gains, out_cotangent):
    place = Place(n, size)
    t = place.t
    model_width = block_in.shape[1]
    width = w_query.shape[1] // 2
    heads = width // HD
    own_rows = block_in.shape[0]
    rows = own_rows * place.group
    assert size == 4 and n % 2 == 0 and rows == 2 * LEN and segment_ids.shape[0] == LEN
    gain_values = gains.astype(F32)
    first_col = (2 * t + place.y) * width
    head_gains = lax.dynamic_slice_in_dim(gain_values, first_col, width, 1)
    positions = jnp.concatenate([(t ^ j) * own_rows + jnp.arange(own_rows, dtype=jnp.int32) for j in range(size)])
    cosine, sine = rope_tables(jnp.concatenate([positions, positions]))
    t_arr = t.reshape(1).astype(jnp.int32)

    def halves(w):
        half = w.shape[1] // 2
        return [lax.dynamic_slice_in_dim(w, c * half, half, 1) for c in (place.y, 1 - place.y)]

    attn_parts = [halves(w) for w in (w_query, w_key, w_value, w_out)]
    attn_mine, attn_theirs = (jnp.concatenate([p[i] for p in attn_parts], axis=1) for i in (0, 1))
    attn_full = line_gather(place, attn_mine, attn_theirs, "wa")
    gate_full = line_gather(place, *halves(w_gate), "wg")
    up_full = line_gather(place, *halves(w_up), "wu")
    down_full = line_gather(place, *halves(w_down), "wd")
    out_full = attn_full[:, 3 * width :]
    ids = jnp.stack([segment_ids, place.swap(segment_ids, size)])

    gathered_in = gather_rows(place, block_in, "xi")
    query_raw = dot_plain(gathered_in, attn_full[:, :width])
    key_raw = dot_plain(gathered_in, attn_full[:, width : 2 * width])
    value_low = dot_plain(gathered_in, attn_full[:, 2 * width : 3 * width]).astype(BF16)
    squares = sum_rows(
        place, jnp.stack([jnp.sum(query_raw * query_raw, axis=1), jnp.sum(key_raw * key_raw, axis=1)]), "ss"
    )
    scales = lax.rsqrt(squares / model_width + EPSILON)
    query_scale, key_scale = scales[0][:, None], scales[1][:, None]
    query_unit = query_raw * query_scale
    key_unit = key_raw * key_scale
    query_rot = rotary((query_unit * head_gains[0]).reshape(rows, heads, HD), cosine, sine)
    key_rot = rotary((key_unit * head_gains[1]).reshape(rows, heads, HD), cosine, sine)
    query_rot = query_rot.reshape(rows, width).astype(BF16)
    key_rot = key_rot.reshape(rows, width).astype(BF16)
    context_low, lse = attention_forward(t_arr, ids, query_rot, key_rot, value_low, size)
    attn_sum = scatter_rows(place, dot_rows(context_low, out_full).astype(BF16), "sa")
    attn_scale = lax.rsqrt(jnp.mean(attn_sum * attn_sum, axis=1, keepdims=True) + EPSILON)
    attn_unit = attn_sum * attn_scale
    hidden_mid = block_in.astype(F32) + attn_unit * gain_values[2]
    hidden_group = gather_rows(place, hidden_mid.astype(BF16), "xh")
    gate_raw = dot_plain(hidden_group, gate_full)
    up_raw = dot_plain(hidden_group, up_full)
    sigmoid_gate = jax.nn.sigmoid(gate_raw)
    silu_gate = gate_raw * sigmoid_gate
    inner_low = (silu_gate * up_raw).astype(BF16)
    mlp_sum = scatter_rows(place, dot_rows(inner_low, down_full).astype(BF16), "sm")
    mlp_scale = lax.rsqrt(jnp.mean(mlp_sum * mlp_sum, axis=1, keepdims=True) + EPSILON)
    mlp_unit = mlp_sum * mlp_scale
    block_out = (hidden_mid + mlp_unit * gain_values[3]).astype(BF16)

    grad_final = out_cotangent.astype(F32)
    mlp_gain_term = jnp.sum(grad_final * mlp_unit, axis=0)
    mixed_back = norm_back(mlp_unit, mlp_scale, grad_final * gain_values[3]).astype(BF16)
    mixed_group = gather_rows(place, mixed_back, "xm")
    down_grad = dot_cols(mixed_group, inner_low).astype(BF16)
    mixed_group, down_grad = lax.optimization_barrier((mixed_group, down_grad))
    down_sum = line_scatter(place, down_grad, "gd")
    inner_back = dot_plain(mixed_group, down_full)
    gate_back = (inner_back * up_raw * sigmoid_gate * (1.0 + gate_raw * (1.0 - sigmoid_gate))).astype(BF16)
    up_back = (inner_back * silu_gate).astype(BF16)
    gate_grad = dot_cols(hidden_group, gate_back).astype(BF16)
    up_grad = dot_cols(hidden_group, up_back).astype(BF16)
    hidden_terms = dot_rows(gate_back, gate_full) + dot_rows(up_back, up_full)
    hidden_sum = scatter_rows(place, hidden_terms.astype(BF16), "sh")
    hidden_sum, gate_grad, up_grad = lax.optimization_barrier((hidden_sum, gate_grad, up_grad))
    gate_sum = line_scatter(place, gate_grad, "gg")
    up_sum = line_scatter(place, up_grad, "gu")
    hidden_back = grad_final + hidden_sum
    attn_gain_term = jnp.sum(hidden_back * attn_unit, axis=0)
    attention_back = norm_back(attn_unit, attn_scale, hidden_back * gain_values[2]).astype(BF16)
    attention_group = gather_rows(place, attention_back, "xa")
    context_back = dot_plain(attention_group, out_full).astype(BF16)
    output_grad = dot_cols(attention_group, context_low).astype(BF16)
    context_back, output_grad = lax.optimization_barrier((context_back, output_grad))
    output_sum = line_scatter(place, output_grad, "go")
    rot_query_back, rot_key_back, value_back = attention_backward(
        t_arr, ids, query_rot, key_rot, value_low, context_back, lse, size
    )
    query_norm_back = unrotary(rot_query_back.reshape(rows, heads, HD), cosine, sine).reshape(rows, width)
    key_norm_back = unrotary(rot_key_back.reshape(rows, heads, HD), cosine, sine).reshape(rows, width)
    query_gain_term = jnp.sum(query_norm_back * query_unit, axis=0)
    key_gain_term = jnp.sum(key_norm_back * key_unit, axis=0)
    query_unit_back = query_norm_back * head_gains[0]
    key_unit_back = key_norm_back * head_gains[1]
    dots = sum_rows(
        place,
        jnp.stack([jnp.sum(query_unit_back * query_unit, axis=1), jnp.sum(key_unit_back * key_unit, axis=1)]),
        "sd",
    )
    query_back = (query_scale * (query_unit_back - query_unit * (dots[0] / model_width)[:, None])).astype(BF16)
    key_back = (key_scale * (key_unit_back - key_unit * (dots[1] / model_width)[:, None])).astype(BF16)
    joint_back = jnp.concatenate([query_back, key_back, value_back], axis=1)
    joint_grad = dot_cols(gathered_in, joint_back).astype(BF16)
    joint_back, joint_grad = lax.optimization_barrier((joint_back, joint_grad))
    joint_sum = line_scatter(place, joint_grad, "gj")
    input_terms = dot_rows(joint_back, attn_full[:, : 3 * width])
    input_grad = (hidden_back + scatter_rows(place, input_terms.astype(BF16), "si")).astype(BF16)

    head_terms = jnp.stack([query_gain_term, key_gain_term])
    placed = lax.dynamic_update_slice(jnp.zeros((2, model_width), F32), head_terms, (jnp.int32(0), first_col))
    gain_terms = jnp.concatenate([placed, jnp.stack([attn_gain_term, mlp_gain_term])], axis=0)
    gains_grad = sum_all(place, gain_terms)

    def joined(sums, first=0, count=None):
        return jnp.concatenate([x[:, first:][:, :count] for x in sums], axis=1)

    return (
        block_out,
        input_grad,
        joined(joint_sum, 0, width),
        joined(joint_sum, width, width),
        joined(joint_sum, 2 * width, width),
        joined(output_sum),
        joined(gate_sum),
        joined(up_sum),
        joined(down_sum),
        gains_grad,
    )


def solution(mesh):
    both = P(("fsdp", "tp"), None)
    weight = P("fsdp", "tp")
    in_specs = (both, P("fsdp"), *[weight] * 7, P(), both)
    out_specs = (both, both, *[weight] * 7, P())
    body = functools.partial(local, mesh.shape["fsdp"], mesh.shape["tp"])
    return jax.shard_map(body, mesh=mesh, in_specs=in_specs, out_specs=out_specs, check_vma=False)
```

```python
import functools

import jax
import jax.numpy as jnp
import numpy as np
from jax import lax
from jax.experimental import pallas as pl
from jax.experimental.pallas import tpu as pltpu
from jax.sharding import PartitionSpec as P


HD = 128
LEN = 1024
SEG_MAX = 512
BLOCK = 256

EPSILON = 1e-06
THETA = 500000.0
NEG_LARGE = -1e30
F32 = jnp.float32
BF16 = jnp.bfloat16


def dot_plain(left, right):
    return jnp.dot(left, right, preferred_element_type=F32)


def dot_rows(left, right):
    return lax.dot_general(left, right, (((1,), (1,)), ((), ())), preferred_element_type=F32)


def dot_cols(left, right):
    return lax.dot_general(left, right, (((0,), (0,)), ((), ())), preferred_element_type=F32)


class Place:
    def __init__(self, n, size):
        self.n, self.size, self.line, self.group = n, size, n // 2, 2 * size
        f, self.t = lax.axis_index("fsdp"), lax.axis_index("tp")
        self.a, self.y = f // 2, f % 2

    def swap(self, x, bit):
        if bit < self.size:
            return lax.ppermute(x, "tp", [(i, i ^ bit) for i in range(self.size)])
        return lax.ppermute(x, "fsdp", [(i, i ^ 1) for i in range(self.n)])

    def lines(self):
        return [[2 * a + y for a in range(self.line)] for y in (0, 1)]


def line_gather(place, mine, theirs):
    other = place.swap(theirs, place.size)
    first = place.y == 0
    shard = jnp.concatenate([jnp.where(first, mine, other), jnp.where(first, other, mine)], axis=0)
    return lax.all_gather(shard, "fsdp", axis=0, tiled=True, axis_index_groups=place.lines())


def line_scatter(place, terms):
    total = lax.psum_scatter(terms, "fsdp", scatter_dimension=0, tiled=True, axis_index_groups=place.lines())
    half = total.shape[0] // 2
    keep = lax.dynamic_slice_in_dim(total, place.y * half, half, 0)
    give = lax.dynamic_slice_in_dim(total, (1 - place.y) * half, half, 0)
    got = place.swap(give, place.size)
    first = place.y == 0
    keep, got = keep.astype(F32), got.astype(F32)
    return jnp.where(first, keep, got), jnp.where(first, got, keep)


def gather_rows(place, own):
    half = own.shape[0] // 2
    b2 = place.swap(own, 2)
    b4 = place.swap(own, 4)
    b1 = place.swap(own, 1)
    b6a = place.swap(b4[:half], 2)
    b6b = place.swap(b2[half:], 4)
    b3 = place.swap(b2, 1)
    b5 = place.swap(b4, 1)
    b6 = jnp.concatenate([b6a, b6b], axis=0)
    b7 = place.swap(b6, 1)
    return jnp.concatenate([own, b1, b2, b3, b4, b5, b6, b7], axis=0)


def scatter_rows(place, terms):
    rows = terms.shape[0] // place.group
    half = rows // 2
    block = [terms[j * rows : (j + 1) * rows] for j in range(place.group)]
    pair = {}
    for j in (6, 2, 4, 0):
        pair[j] = block[j].astype(F32) + place.swap(block[j + 1], 1).astype(F32)
    corner = pair[6].astype(BF16)
    via_x = place.swap(corner[:half], 2).astype(F32)
    via_y = place.swap(corner[half:], 4).astype(F32)
    from_x = place.swap((pair[2] + jnp.pad(via_y, ((half, 0), (0, 0)))).astype(BF16), 2)
    from_y = place.swap((pair[4] + jnp.pad(via_x, ((0, half), (0, 0)))).astype(BF16), 4)
    return pair[0] + from_x.astype(F32) + from_y.astype(F32)


def sum_rows(place, values):
    m, total = values.shape
    v = values.reshape(m, place.group, total // place.group)
    for bit in (1, 2, 4):
        got = place.swap(v, bit)
        v = v + got[:, np.arange(place.group) ^ bit]
    return v.reshape(m, total)


def sum_all(place, values):
    for bit in (1, 2, 4):
        values = values + place.swap(values, bit)
    bit = 2
    while bit < place.n:
        values = values + lax.ppermute(values, "fsdp", [(i, i ^ bit) for i in range(place.n)])
        bit *= 2
    return values


def rel_block(t, c, rows):
    return pl.ds(pl.multiple_of((t ^ c) * rows, rows), rows)


def in_order(ref, t, count, rows):
    return jnp.concatenate([ref[rel_block(t, c, rows), :] for c in range(count)], axis=0)


def visible_block(c, lo, hi, ids_col, ids_row):
    q_pos = c * BLOCK + lax.broadcasted_iota(jnp.int32, (BLOCK, hi - lo), 0)
    k_pos = lo + lax.broadcasted_iota(jnp.int32, (BLOCK, hi - lo), 1)
    same = ids_col[c * BLOCK : (c + 1) * BLOCK, :] == ids_row[:, lo:hi]
    return same & (k_pos <= q_pos)


def key_range(c):
    first = max(0, c * BLOCK - SEG_MAX + 1) // BLOCK * BLOCK
    return first, (c + 1) * BLOCK


def attend_kernel(count, rows, t_ref, ids_col, ids_row, q_ref, k_ref, v_ref, ctx_ref, lse_ref):
    t = t_ref[0]
    q = in_order(q_ref, t, count, rows)
    k = in_order(k_ref, t, count, rows)
    v = in_order(v_ref, t, count, rows)
    per = rows // BLOCK
    for c in range(count * per):
        lo, hi = key_range(c)
        at = pl.ds(pl.multiple_of((t ^ (c // per)) * rows + c % per * BLOCK, BLOCK), BLOCK)
        scores = dot_rows(q[c * BLOCK : (c + 1) * BLOCK], k[lo:hi]) * HD ** (-0.5)
        scores = jnp.where(visible_block(c, lo, hi, ids_col, ids_row), scores, NEG_LARGE)
        top = jnp.max(scores, axis=-1, keepdims=True)
        exponent = jnp.exp(scores - top)
        total = jnp.sum(exponent, axis=-1, keepdims=True)
        probs = (exponent * (1.0 / total)).astype(BF16)
        ctx_ref[at, :] = dot_plain(probs, v[lo:hi]).astype(BF16)
        lse_ref[0, at, :] = top + jnp.log(total)


def attend_back_kernel(
    count, rows, t_ref, ids_col, ids_row, q_ref, k_ref, v_ref, g_ref, lse_ref, dq_ref, dk_ref, dv_ref, dk_acc, dv_acc
):
    t = t_ref[0]
    q = in_order(q_ref, t, count, rows)
    k = in_order(k_ref, t, count, rows)
    v = in_order(v_ref, t, count, rows)
    g = in_order(g_ref, t, count, rows)
    dk_acc[...] = jnp.zeros_like(dk_acc)
    dv_acc[...] = jnp.zeros_like(dv_acc)
    per = rows // BLOCK
    for c in range(count * per):
        lo, hi = key_range(c)
        at = pl.ds(pl.multiple_of((t ^ (c // per)) * rows + c % per * BLOCK, BLOCK), BLOCK)
        q_c, g_c = q[c * BLOCK : (c + 1) * BLOCK], g[c * BLOCK : (c + 1) * BLOCK]
        scores = dot_rows(q_c, k[lo:hi]) * HD ** (-0.5)
        seen = visible_block(c, lo, hi, ids_col, ids_row)
        probs = jnp.where(seen, jnp.exp(jnp.where(seen, scores, NEG_LARGE) - lse_ref[0, at, :]), 0.0)
        probs_back = dot_rows(g_c, v[lo:hi])
        delta = jnp.sum(probs * probs_back, axis=-1, keepdims=True)
        scores_back = (probs * (probs_back - delta)).astype(BF16)
        dq_ref[at, :] = dot_plain(scores_back, k[lo:hi]) * HD ** (-0.5)
        dk_acc[lo:hi, :] += dot_cols(scores_back, q_c)
        dv_acc[lo:hi, :] += dot_cols(probs.astype(BF16), g_c)
    for c in range(count):
        dk_ref[rel_block(t, c, rows), :] = dk_acc[c * rows : (c + 1) * rows, :] * HD ** (-0.5)
        dv_ref[rel_block(t, c, rows), :] = dv_acc[c * rows : (c + 1) * rows, :].astype(BF16)


def attention_forward(t, ids, q, k, v, count):
    seqs, length = ids.shape
    width = q.shape[1]
    heads = width // HD
    col = pl.BlockSpec((length, HD), lambda s, h, t: (s, h))
    spec = pltpu.PrefetchScalarGridSpec(
        num_scalar_prefetch=1,
        grid=(seqs, heads),
        in_specs=[
            pl.BlockSpec((length, 1), lambda s, h, t: (s, 0)),
            pl.BlockSpec((pl.Squeezed(), 1, length), lambda s, h, t: (s, 0, 0)),
            col,
            col,
            col,
        ],
        out_specs=[col, pl.BlockSpec((1, length, 1), lambda s, h, t: (h, s, 0))],
    )
    return pl.pallas_call(
        functools.partial(attend_kernel, count, length // count),
        out_shape=[
            jax.ShapeDtypeStruct((seqs * length, width), BF16),
            jax.ShapeDtypeStruct((heads, seqs * length, 1), F32),
        ],
        grid_spec=spec,
        cost_estimate=pl.CostEstimate(
            flops=4 * seqs * length * length * width,
            bytes_accessed=8 * seqs * length * width,
            transcendentals=seqs * heads * length * length,
        ),
        name="attend",
    )(t, ids.reshape(-1, 1), ids.reshape(seqs, 1, length), q, k, v)


def attention_backward(t, ids, q, k, v, g, lse, count):
    seqs, length = ids.shape
    width = q.shape[1]
    heads = width // HD
    col = pl.BlockSpec((length, HD), lambda s, h, t: (s, h))
    spec = pltpu.PrefetchScalarGridSpec(
        num_scalar_prefetch=1,
        grid=(seqs, heads),
        in_specs=[
            pl.BlockSpec((length, 1), lambda s, h, t: (s, 0)),
            pl.BlockSpec((pl.Squeezed(), 1, length), lambda s, h, t: (s, 0, 0)),
            col,
            col,
            col,
            col,
            pl.BlockSpec((1, length, 1), lambda s, h, t: (h, s, 0)),
        ],
        out_specs=[col, col, col],
        scratch_shapes=[pltpu.VMEM((length, HD), F32), pltpu.VMEM((length, HD), F32)],
    )
    return pl.pallas_call(
        functools.partial(attend_back_kernel, count, length // count),
        out_shape=[
            jax.ShapeDtypeStruct((seqs * length, width), F32),
            jax.ShapeDtypeStruct((seqs * length, width), F32),
            jax.ShapeDtypeStruct((seqs * length, width), BF16),
        ],
        grid_spec=spec,
        cost_estimate=pl.CostEstimate(
            flops=10 * seqs * length * length * width,
            bytes_accessed=18 * seqs * length * width,
            transcendentals=seqs * heads * length * length,
        ),
        name="attend_back",
    )(t, ids.reshape(-1, 1), ids.reshape(seqs, 1, length), q, k, v, g, lse)


def rotate_half(values):
    front_half = values[..., : HD // 2]
    back_half = values[..., HD // 2 :]
    return jnp.concatenate([-back_half, front_half], axis=-1)


def rotate_back(values):
    front_half = values[..., : HD // 2]
    back_half = values[..., HD // 2 :]
    return jnp.concatenate([back_half, -front_half], axis=-1)


def rotary(values, cosine, sine):
    return values * cosine + rotate_half(values) * sine


def unrotary(values, cosine, sine):
    return values * cosine + rotate_back(values * sine)


def rope_tables(positions):
    freq_index = jnp.arange(HD // 2, dtype=F32)
    frequency = THETA ** (-2.0 * freq_index / HD)
    angles = positions.astype(F32)[:, None] * frequency[None, :]
    angles = jnp.concatenate([angles, angles], axis=1)[:, None, :]
    return jnp.cos(angles), jnp.sin(angles)


def norm_back(unit_rows, scales, grad_unit):
    return scales * (grad_unit - unit_rows * jnp.mean(grad_unit * unit_rows, axis=-1, keepdims=True))


def local(n, size, block_in, segment_ids, w_query, w_key, w_value, w_out, w_gate, w_up, w_down, gains, out_cotangent):
    place = Place(n, size)
    t = place.t
    model_width = block_in.shape[1]
    width = w_query.shape[1] // 2
    heads = width // HD
    own_rows = block_in.shape[0]
    rows = own_rows * place.group
    assert size == 4 and n % 2 == 0 and rows == 2 * LEN and segment_ids.shape[0] == LEN
    gain_values = gains.astype(F32)
    first_col = (2 * t + place.y) * width
    head_gains = lax.dynamic_slice_in_dim(gain_values, first_col, width, 1)
    positions = jnp.concatenate([(t ^ j) * own_rows + jnp.arange(own_rows, dtype=jnp.int32) for j in range(size)])
    cosine, sine = rope_tables(jnp.concatenate([positions, positions]))
    t_arr = t.reshape(1).astype(jnp.int32)

    def halves(w):
        half = w.shape[1] // 2
        return [lax.dynamic_slice_in_dim(w, c * half, half, 1) for c in (place.y, 1 - place.y)]

    attn_parts = [halves(w) for w in (w_query, w_key, w_value, w_out)]
    attn_mine, attn_theirs = (jnp.concatenate([p[i] for p in attn_parts], axis=1) for i in (0, 1))
    attn_full = line_gather(place, attn_mine, attn_theirs)
    gate_full = line_gather(place, *halves(w_gate))
    up_full = line_gather(place, *halves(w_up))
    down_full = line_gather(place, *halves(w_down))
    out_full = attn_full[:, 3 * width :]
    ids = jnp.stack([segment_ids, place.swap(segment_ids, size)])

    gathered_in = gather_rows(place, block_in)
    query_raw = dot_plain(gathered_in, attn_full[:, :width])
    key_raw = dot_plain(gathered_in, attn_full[:, width : 2 * width])
    row_squares = jnp.stack([jnp.sum(query_raw * query_raw, axis=1), jnp.sum(key_raw * key_raw, axis=1)])
    value_low = dot_plain(gathered_in, attn_full[:, 2 * width : 3 * width]).astype(BF16)
    squares = sum_rows(place, row_squares)
    scales = lax.rsqrt(squares / model_width + EPSILON)
    query_scale, key_scale = scales[0][:, None], scales[1][:, None]
    query_unit = query_raw * query_scale
    key_unit = key_raw * key_scale
    query_rot = rotary((query_unit * head_gains[0]).reshape(rows, heads, HD), cosine, sine)
    key_rot = rotary((key_unit * head_gains[1]).reshape(rows, heads, HD), cosine, sine)
    query_rot = query_rot.reshape(rows, width).astype(BF16)
    key_rot = key_rot.reshape(rows, width).astype(BF16)
    context_low, lse = attention_forward(t_arr, ids, query_rot, key_rot, value_low, size)
    attn_sum = scatter_rows(place, dot_rows(context_low, out_full).astype(BF16))
    attn_scale = lax.rsqrt(jnp.mean(attn_sum * attn_sum, axis=1, keepdims=True) + EPSILON)
    attn_unit = attn_sum * attn_scale
    hidden_mid = block_in.astype(F32) + attn_unit * gain_values[2]
    hidden_group = gather_rows(place, hidden_mid.astype(BF16))
    gate_raw = dot_plain(hidden_group, gate_full)
    up_raw = dot_plain(hidden_group, up_full)
    sigmoid_gate = jax.nn.sigmoid(gate_raw)
    silu_gate = gate_raw * sigmoid_gate
    inner_low = (silu_gate * up_raw).astype(BF16)
    mlp_sum = scatter_rows(place, dot_rows(inner_low, down_full).astype(BF16))
    mlp_scale = lax.rsqrt(jnp.mean(mlp_sum * mlp_sum, axis=1, keepdims=True) + EPSILON)
    mlp_unit = mlp_sum * mlp_scale
    block_out = (hidden_mid + mlp_unit * gain_values[3]).astype(BF16)

    grad_final = out_cotangent.astype(F32)
    mlp_gain_term = jnp.sum(grad_final * mlp_unit, axis=0)
    mixed_back = norm_back(mlp_unit, mlp_scale, grad_final * gain_values[3]).astype(BF16)
    mixed_group = gather_rows(place, mixed_back)
    down_grad = dot_cols(mixed_group, inner_low).astype(BF16)
    mixed_group, down_grad = lax.optimization_barrier((mixed_group, down_grad))
    down_sum = line_scatter(place, down_grad)
    inner_back = dot_plain(mixed_group, down_full)
    gate_back = (inner_back * up_raw * sigmoid_gate * (1.0 + gate_raw * (1.0 - sigmoid_gate))).astype(BF16)
    up_back = (inner_back * silu_gate).astype(BF16)
    gate_grad = dot_cols(hidden_group, gate_back).astype(BF16)
    up_grad = dot_cols(hidden_group, up_back).astype(BF16)
    hidden_terms = dot_rows(gate_back, gate_full) + dot_rows(up_back, up_full)
    hidden_sum = scatter_rows(place, hidden_terms.astype(BF16))
    hidden_sum, gate_grad, up_grad = lax.optimization_barrier((hidden_sum, gate_grad, up_grad))
    gate_sum = line_scatter(place, gate_grad)
    up_sum = line_scatter(place, up_grad)
    hidden_back = grad_final + hidden_sum
    attn_gain_term = jnp.sum(hidden_back * attn_unit, axis=0)
    attention_back = norm_back(attn_unit, attn_scale, hidden_back * gain_values[2]).astype(BF16)
    attention_group = gather_rows(place, attention_back)
    context_back = dot_plain(attention_group, out_full).astype(BF16)
    output_grad = dot_cols(attention_group, context_low).astype(BF16)
    context_back, output_grad = lax.optimization_barrier((context_back, output_grad))
    output_sum = line_scatter(place, output_grad)
    rot_query_back, rot_key_back, value_back = attention_backward(
        t_arr, ids, query_rot, key_rot, value_low, context_back, lse, size
    )
    query_norm_back = unrotary(rot_query_back.reshape(rows, heads, HD), cosine, sine).reshape(rows, width)
    key_norm_back = unrotary(rot_key_back.reshape(rows, heads, HD), cosine, sine).reshape(rows, width)
    query_gain_term = jnp.sum(query_norm_back * query_unit, axis=0)
    key_gain_term = jnp.sum(key_norm_back * key_unit, axis=0)
    query_unit_back = query_norm_back * head_gains[0]
    key_unit_back = key_norm_back * head_gains[1]
    dots = sum_rows(
        place, jnp.stack([jnp.sum(query_unit_back * query_unit, axis=1), jnp.sum(key_unit_back * key_unit, axis=1)])
    )
    query_back = (query_scale * (query_unit_back - query_unit * (dots[0] / model_width)[:, None])).astype(BF16)
    key_back = (key_scale * (key_unit_back - key_unit * (dots[1] / model_width)[:, None])).astype(BF16)
    joint_back = jnp.concatenate([query_back, key_back, value_back], axis=1)
    joint_grad = dot_cols(gathered_in, joint_back).astype(BF16)
    joint_back, joint_grad = lax.optimization_barrier((joint_back, joint_grad))
    joint_sum = line_scatter(place, joint_grad)
    input_terms = dot_rows(joint_back, attn_full[:, : 3 * width])
    input_grad = (hidden_back + scatter_rows(place, input_terms.astype(BF16))).astype(BF16)

    head_terms = jnp.stack([query_gain_term, key_gain_term])
    placed = lax.dynamic_update_slice(jnp.zeros((2, model_width), F32), head_terms, (jnp.int32(0), first_col))
    gain_terms = jnp.concatenate([placed, jnp.stack([attn_gain_term, mlp_gain_term])], axis=0)
    gains_grad = sum_all(place, gain_terms)

    def joined(sums, first=0, count=None):
        return jnp.concatenate([x[:, first:][:, :count] for x in sums], axis=1)

    return (
        block_out,
        input_grad,
        joined(joint_sum, 0, width),
        joined(joint_sum, width, width),
        joined(joint_sum, 2 * width, width),
        joined(output_sum),
        joined(gate_sum),
        joined(up_sum),
        joined(down_sum),
        gains_grad,
    )


def solution(mesh):
    both = P(("fsdp", "tp"), None)
    weight = P("fsdp", "tp")
    in_specs = (both, P("fsdp"), *[weight] * 7, P(), both)
    out_specs = (both, both, *[weight] * 7, P())

    def body(*args):
        return local(mesh.shape["fsdp"], mesh.shape["tp"], *args)

    return jax.shard_map(body, mesh=mesh, in_specs=in_specs, out_specs=out_specs, check_vma=False)
```
